32 devices in a mesh: seq: 16 (over z, y, x), bat: 2 (over core).
Axes of the slice: x: 2, y: 2, z: 4, core: 2. Of those that a mesh axis runs over, the one named last changes fastest.
Arguments:
- tokens: bfloat16 [2, 65536, 256], P('bat', 'seq'), may hold values from -6 to 6
- filter_spectrum: bfloat16 [2, 256, 256, 256], P(None, 'seq', None, 'bat'), may hold values from -6 to 6
- skip_gain: float32 [256], replicated, may hold values from 0.5 to 1.5
Outputs:
- mixed: bfloat16 [2, 65536, 256], P('bat', 'seq')
The draws below stay inside these ranges and needn't reach their ends.
All inputs are finite; a program needn't handle non-finite values.
Results may differ from the reference program's by a relative error of at most 0.012.
Values may be sent and summed in bfloat16 or wider, within the bound.
No kernel may reach another device: no remote copies, remote signals or barrier semaphores. Data moves between devices by JAX's collectives and lax.ppermute only.
A program may use at most 64 MiB of HBM per device.

```python
import math
import jax
import jax.numpy as jnp
from jax import lax

C = 256
N1 = 256
N2 = 256
BATCH = 2
LENGTH = 65536


def level_of(own_key, shape, pieces, least, largest):
    def one(dim, parts):
        steps = jax.random.uniform(jax.random.fold_in(jax.random.fold_in(own_key, 6), dim), (parts,), jnp.float32, least / len(pieces), largest / len(pieces))
        return jnp.repeat(jnp.exp(steps), shape[dim] // parts).reshape((-1,) + (1,) * (len(shape) - dim - 1))

    gain = one(*pieces[0])
    for cut in pieces[1:]:
        gain = gain * one(*cut)
    return gain


def noise(key, shape, scale, most, shards=(), kind=jnp.bfloat16):
    array = jax.random.normal(key, shape, jnp.float32) * scale
    if len(shards) > 0:
        array = level_of(key, shape, shards, -0.22, 0.18) * array
    return jnp.clip(array, min=-most, max=most).astype(kind)


def setup_inputs(seed: int = 0) -> dict:
    key_of = jax.random.split(jax.random.key(seed), 4)
    return {
        "tokens": noise(key_of[0], (BATCH, LENGTH, C), 1.0, 6.0, ((0, 2), (1, 16))),
        "filter_spectrum": noise(key_of[1], (2, N1, N2, C), 1.0, 6.0, ((1, 16), (3, 2))),
        "skip_gain": jnp.clip(jax.random.uniform(key_of[2], (C,), jnp.float32, 0.5, 1.5), 0.5, 1.5),
    }


def cos_sin(points):
    steps_range = jnp.arange(points, dtype=jnp.int32)
    index_grid = (steps_range[:, None] * steps_range[None, :]) % points
    phase_angle = index_grid.astype(jnp.float32) * (2.0 * math.pi / points)
    return jnp.cos(phase_angle), jnp.sin(phase_angle)


def real_table(points):
    cosine, sine_vals = cos_sin(points)
    return jnp.stack([cosine, -sine_vals], axis=1).astype(jnp.bfloat16)


def complex_table(points, signum, factor):
    cosine, sine_vals = cos_sin(points)
    top_rows = jnp.stack([cosine, signum * sine_vals], axis=1)
    low_rows = jnp.stack([-signum * sine_vals, cosine], axis=1)
    return (jnp.stack([top_rows, low_rows], axis=0) * factor).astype(jnp.bfloat16)


def final_table(points):
    cosine, sine_vals = cos_sin(points)
    return (jnp.stack([cosine, -sine_vals], axis=0) / points).astype(jnp.bfloat16)


def twiddle_phase(first_rows, second_rows, period):
    index_grid = (first_rows[:, None] * second_rows[None, :]) % period
    phase_angle = index_grid.astype(jnp.float32) * (2.0 * math.pi / period)
    return jnp.cos(phase_angle)[..., None], jnp.sin(phase_angle)[..., None]


def round_half(values):
    return lax.optimization_barrier(values.astype(jnp.bfloat16)).astype(jnp.float32)


def reference(tokens, filter_spectrum, skip_gain):
    period = N1 * N2
    forward_rows = real_table(N1).astype(jnp.float32)
    forward_cols = complex_table(N2, -1.0, 1.0).astype(jnp.float32)
    inverse_cols = complex_table(N2, 1.0, 1.0 / N2).astype(jnp.float32)
    inverse_rows = final_table(N1).astype(jnp.float32)
    cos_tw, sin_tw = twiddle_phase(jnp.arange(N1, dtype=jnp.int32), jnp.arange(N2, dtype=jnp.int32), period)
    filters_f32 = filter_spectrum.astype(jnp.float32)

    def one_sequence(sequence):
        columns = sequence.reshape(N1, N2, C).astype(jnp.float32)
        first_section = jnp.einsum("nmc,nsk->skmc", columns, forward_rows)
        real_part = first_section[0] * cos_tw + first_section[1] * sin_tw
        imag_part = first_section[1] * cos_tw - first_section[0] * sin_tw
        turned = round_half(jnp.stack([real_part, imag_part]))
        spectrum = round_half(jnp.einsum("rknc,rnsj->skjc", turned, forward_cols))
        prod_real = spectrum[0] * filters_f32[0] - spectrum[1] * filters_f32[1]
        prod_imag = spectrum[0] * filters_f32[1] + spectrum[1] * filters_f32[0]
        product = round_half(jnp.stack([prod_real, prod_imag]))
        back_section = jnp.einsum("rkjc,rjsn->sknc", product, inverse_cols)
        real_back = back_section[0] * cos_tw - back_section[1] * sin_tw
        imag_back = back_section[0] * sin_tw + back_section[1] * cos_tw
        turned_back = round_half(jnp.stack([real_back, imag_back]))
        filtered = jnp.einsum("rknc,rkm->mnc", turned_back, inverse_rows)
        result = filtered + skip_gain * columns
        return result.astype(jnp.bfloat16).reshape(N1 * N2, C)

    return lax.map(one_sequence, tokens)
```

```python
import functools
import math

import jax
import jax.numpy as jnp
from jax import lax
from jax.experimental import pallas as pl
from jax.experimental.pallas import tpu as pltpu
from jax.sharding import PartitionSpec as P

N1 = 256
N2 = 256


def cos_sin(points):
    steps_range = jnp.arange(points, dtype=jnp.int32)
    index_grid = steps_range[:, None] * steps_range[None, :] % points
    phase_angle = index_grid.astype(jnp.float32) * (2.0 * math.pi / points)
    return (jnp.cos(phase_angle), jnp.sin(phase_angle))


def dft_tables():
    cos1, sin1 = cos_sin(N1)
    cos2, sin2 = cos_sin(N2)
    forward_rows = jnp.stack([cos1, -sin1]).astype(jnp.bfloat16)
    top = jnp.concatenate([cos2, -sin2], axis=1)
    low = jnp.concatenate([sin2, cos2], axis=1)
    forward_cols = jnp.stack([top, low]).astype(jnp.bfloat16)
    top = jnp.concatenate([cos2, sin2], axis=1)
    low = jnp.concatenate([-sin2, cos2], axis=1)
    inverse_cols = (jnp.stack([top, low]) / N2).astype(jnp.bfloat16)
    inverse_rows = (jnp.stack([cos1, -sin1]) / N1).astype(jnp.bfloat16)
    period = N1 * N2
    rows = jnp.arange(N1, dtype=jnp.int32)
    cols = jnp.arange(N2, dtype=jnp.int32)
    angle = (rows[:, None] * cols[None, :] % period).astype(jnp.float32) * (2.0 * math.pi / period)
    twiddle = jnp.stack([jnp.cos(angle), jnp.sin(angle)])
    return forward_rows, twiddle, forward_cols, inverse_cols, inverse_rows


def dot(left, right):
    return jnp.dot(left, right, preferred_element_type=jnp.float32)


def span(block, step, held):
    if held <= step:
        return pl.ds(block * step // held, step // held), pl.ds(0, held)
    return pl.ds(block * step // held, 1), pl.ds(block * step % held, step)


def convolve_kernel(blocks, gain, tokens, filters, rows_t, twiddle, cols_t, back_t, final_t, out, turned_back):
    signal = tokens[0, :, 0].reshape(N1, N2)
    step = N1 // blocks
    for block in range(blocks):
        rows = pl.ds(block * step, step)
        real = dot(rows_t[0, rows], signal)
        imag = dot(rows_t[1, rows], signal)
        cosine = twiddle[0, rows]
        sine = twiddle[1, rows]
        turned_real = (real * cosine + imag * sine).astype(jnp.bfloat16)
        turned_imag = (imag * cosine - real * sine).astype(jnp.bfloat16)
        spectrum = dot(turned_real, cols_t[0]) + dot(turned_imag, cols_t[1])
        spectrum = spectrum.astype(jnp.bfloat16).astype(jnp.float32)
        parts, inner = span(block, step, filters.shape[3])
        weight_real = filters[parts, 0, 0, inner].reshape(step, N2).astype(jnp.float32)
        weight_imag = filters[parts, 0, 1, inner].reshape(step, N2).astype(jnp.float32)
        spec_real, spec_imag = spectrum[:, :N2], spectrum[:, N2:]
        prod_real = (spec_real * weight_real - spec_imag * weight_imag).astype(jnp.bfloat16)
        prod_imag = (spec_real * weight_imag + spec_imag * weight_real).astype(jnp.bfloat16)
        back = dot(prod_real, back_t[0]) + dot(prod_imag, back_t[1])
        back_real, back_imag = back[:, :N2], back[:, N2:]
        turned_back[0, rows] = (back_real * cosine - back_imag * sine).astype(jnp.bfloat16)
        turned_back[1, rows] = (back_real * sine + back_imag * cosine).astype(jnp.bfloat16)
    weight = gain[pl.program_id(0)]
    for block in range(blocks):
        rows = pl.ds(block * step, step)
        parts, inner = span(block, step, tokens.shape[3])
        filtered = dot(final_t[0, rows], turned_back[0]) + dot(final_t[1, rows], turned_back[1])
        direct = tokens[0, parts, 0, inner].reshape(step, N2).astype(jnp.float32)
        result = (filtered + weight * direct).astype(jnp.bfloat16)
        out[0, parts, 0, inner] = result.reshape(parts.size, inner.size, N2)


def convolve(tokens, filters, gain, tables, start, count):
    batch, pieces, _, rows, _ = tokens.shape
    blocks = 2

    def whole(array):
        return pl.BlockSpec(array.shape, lambda c, b: (0,) * array.ndim)

    block = (1, pieces, 1, rows, N2)
    return pl.pallas_call(
        functools.partial(convolve_kernel, blocks),
        grid=(count, batch),
        in_specs=[
            pl.BlockSpec(memory_space=pltpu.SMEM),
            pl.BlockSpec(block, lambda c, b: (b, 0, c + start, 0, 0)),
            pl.BlockSpec((pieces, 1, 2, rows, N2), lambda c, b: (0, c + start, 0, 0, 0)),
            *[whole(table) for table in tables],
        ],
        out_specs=pl.BlockSpec(block, lambda c, b: (b, 0, c, 0, 0)),
        out_shape=jax.ShapeDtypeStruct((batch, pieces, count, rows, N2), jnp.bfloat16),
        scratch_shapes=[pltpu.VMEM((2, N1, N2), jnp.bfloat16)],
        name="convolve",
    )(gain[start : start + count], tokens, filters, *tables)


def body(tokens, filter_spectrum, skip_gain):
    seq_count = lax.axis_size("seq")
    bat_count = lax.axis_size("bat")
    seq_index = lax.axis_index("seq")
    bat_index = lax.axis_index("bat")
    batch_rows, local_length, channels = tokens.shape
    rows_local = N1 // seq_count
    spread = channels % (seq_count * bat_count) == 0
    if spread:
        axes, groups = ("bat", "seq"), bat_count
        own = channels // (seq_count * bat_count)
        first = (bat_index * seq_count + seq_index) * own
        sequences = batch_rows * bat_count
    else:
        axes, groups = ("seq",), 1
        own = channels // seq_count
        first = seq_index * own
        sequences = batch_rows
        filter_spectrum = lax.all_gather(filter_spectrum, "bat", axis=3, tiled=True)
    ranks = seq_count * groups

    laid = tokens.reshape(batch_rows, rows_local, N2, channels).transpose(3, 0, 1, 2)
    laid = laid.reshape(ranks, own, batch_rows, rows_local, N2)
    columns = lax.all_to_all(laid, axes, split_axis=0, concat_axis=0, tiled=True)
    columns = columns.reshape(groups, seq_count, own, batch_rows, rows_local, N2)
    if batch_rows == 1:
        columns = columns.reshape(sequences, seq_count, own, rows_local, N2)
    else:
        columns = columns.transpose(0, 3, 1, 2, 4, 5).reshape(sequences, seq_count, own, rows_local, N2)

    spread_filters = filter_spectrum.transpose(3, 0, 1, 2).reshape(seq_count, own, 2, rows_local, N2)
    filters = lax.all_to_all(spread_filters, "seq", split_axis=0, concat_axis=0, tiled=True)
    gain = lax.dynamic_slice(skip_gain, (first,), (own,))
    tables = dft_tables()
    aligned = rows_local % 16 == 0
    if not aligned:
        columns = columns.transpose(0, 2, 1, 3, 4).reshape(sequences, 1, own, N1, N2)
        filters = filters.transpose(1, 2, 0, 3, 4).reshape(1, own, 2, N1, N2)
    chunks = 2 if own % 2 == 0 else 1
    count = own // chunks
    results = []
    for chunk in range(chunks):
        result = convolve(columns, filters, gain, tables, chunk * count, count)
        if not aligned:
            result = result.reshape(sequences, count, seq_count, rows_local, N2).transpose(0, 2, 1, 3, 4)
        if batch_rows == 1:
            result = result.reshape(ranks, count, 1, rows_local, N2)
        else:
            result = result.reshape(groups, batch_rows, seq_count, count, rows_local, N2)
            result = result.transpose(0, 2, 3, 1, 4, 5).reshape(ranks, count, batch_rows, rows_local, N2)
        results.append(lax.all_to_all(result, axes, split_axis=0, concat_axis=0, tiled=True))
    restored = jnp.concatenate(results, axis=1).reshape(channels, batch_rows, rows_local, N2)
    return restored.transpose(1, 2, 3, 0).reshape(batch_rows, local_length, channels)


def solution(mesh):
    placed = (P("bat", "seq", None), P(None, "seq", None, "bat"), P())
    return jax.shard_map(
        body, mesh=mesh, in_specs=placed, out_specs=P("bat", "seq", None), check_vma=False
    )
```

```python
import functools
import math

import jax
import jax.numpy as jnp
from jax import lax
from jax.experimental import pallas as pl
from jax.experimental.pallas import tpu as pltpu
from jax.sharding import PartitionSpec as P


N1 = 256
N2 = 256


def cos_sin(points):
    steps_range = jnp.arange(points, dtype=jnp.int32)
    index_grid = steps_range[:, None] * steps_range[None, :] % points
    phase_angle = index_grid.astype(jnp.float32) * (2.0 * math.pi / points)
    return (jnp.cos(phase_angle), jnp.sin(phase_angle))


def dft_tables(order):
    index_grid = order[:, None] * order[None, :] % N1
    phase_angle = index_grid.astype(jnp.float32) * (2.0 * math.pi / N1)
    cos1, sin1 = jnp.cos(phase_angle), jnp.sin(phase_angle)
    cos2, sin2 = cos_sin(N2)
    forward_rows = jnp.stack([cos1, -sin1]).astype(jnp.bfloat16)
    top = jnp.concatenate([cos2, -sin2], axis=1)
    low = jnp.concatenate([sin2, cos2], axis=1)
    forward_cols = jnp.stack([top, low]).astype(jnp.bfloat16)
    top = jnp.concatenate([cos2, sin2], axis=1)
    low = jnp.concatenate([-sin2, cos2], axis=1)
    inverse_cols = (jnp.stack([top, low]) / N2).astype(jnp.bfloat16)
    inverse_rows = (jnp.stack([cos1, -sin1]) / N1).astype(jnp.bfloat16)
    period = N1 * N2
    cols = jnp.arange(N2, dtype=jnp.int32)
    angle = (order[:, None] * cols[None, :] % period).astype(jnp.float32) * (2.0 * math.pi / period)
    twiddle = jnp.stack([jnp.cos(angle), jnp.sin(angle)])
    return forward_rows, twiddle, forward_cols, inverse_cols, inverse_rows


def dot(left, right):
    return jnp.dot(left, right, preferred_element_type=jnp.float32)


def span(block, step, held):
    if held <= step:
        return pl.ds(block * step // held, step // held), pl.ds(0, held)
    return pl.ds(block * step // held, 1), pl.ds(block * step % held, step)


def convolve_kernel(blocks, gain, tokens, filters, rows_t, twiddle, cols_t, back_t, final_t, out, turned_back):
    signal = tokens[0, :, 0].reshape(N1, N2)
    step = N1 // blocks
    for block in range(blocks):
        rows = pl.ds(block * step, step)
        real = dot(rows_t[0, rows], signal)
        imag = dot(rows_t[1, rows], signal)
        cosine = twiddle[0, rows]
        sine = twiddle[1, rows]
        turned_real = (real * cosine + imag * sine).astype(jnp.bfloat16)
        turned_imag = (imag * cosine - real * sine).astype(jnp.bfloat16)
        spectrum = dot(turned_real, cols_t[0]) + dot(turned_imag, cols_t[1])
        spectrum = spectrum.astype(jnp.bfloat16).astype(jnp.float32)
        parts, inner = span(block, step, filters.shape[3])
        weight_real = filters[parts, 0, 0, inner].reshape(step, N2).astype(jnp.float32)
        weight_imag = filters[parts, 0, 1, inner].reshape(step, N2).astype(jnp.float32)
        spec_real, spec_imag = spectrum[:, :N2], spectrum[:, N2:]
        prod_real = (spec_real * weight_real - spec_imag * weight_imag).astype(jnp.bfloat16)
        prod_imag = (spec_real * weight_imag + spec_imag * weight_real).astype(jnp.bfloat16)
        back = dot(prod_real, back_t[0]) + dot(prod_imag, back_t[1])
        back_real, back_imag = back[:, :N2], back[:, N2:]
        turned_back[0, rows] = (back_real * cosine - back_imag * sine).astype(jnp.bfloat16)
        turned_back[1, rows] = (back_real * sine + back_imag * cosine).astype(jnp.bfloat16)
    weight = gain[pl.program_id(0)]
    for block in range(blocks):
        rows = pl.ds(block * step, step)
        parts, inner = span(block, step, tokens.shape[3])
        filtered = dot(final_t[0, rows], turned_back[0]) + dot(final_t[1, rows], turned_back[1])
        direct = tokens[0, parts, 0, inner].reshape(step, N2).astype(jnp.float32)
        result = (filtered + weight * direct).astype(jnp.bfloat16)
        out[0, parts, 0, inner] = result.reshape(parts.size, inner.size, N2)


def convolve(tokens, filters, gain, tables, start, count):
    batch, pieces, _, rows, _ = tokens.shape
    blocks = 2

    def whole(array):
        return pl.BlockSpec(array.shape, lambda c, b: (0,) * array.ndim)

    block = (1, pieces, 1, rows, N2)
    return pl.pallas_call(
        functools.partial(convolve_kernel, blocks),
        grid=(count, batch),
        in_specs=[
            pl.BlockSpec(memory_space=pltpu.SMEM),
            pl.BlockSpec(block, lambda c, b: (b, 0, c + start, 0, 0)),
            pl.BlockSpec((pieces, 1, 2, rows, N2), lambda c, b: (0, c + start, 0, 0, 0)),
            *[whole(table) for table in tables],
        ],
        out_specs=pl.BlockSpec(block, lambda c, b: (b, 0, c, 0, 0)),
        out_shape=jax.ShapeDtypeStruct((batch, pieces, count, rows, N2), jnp.bfloat16),
        scratch_shapes=[pltpu.VMEM((2, N1, N2), jnp.bfloat16)],
        name="convolve",
    )(gain[start : start + count], tokens, filters, *tables)


def spread_body(tokens, filter_spectrum, skip_gain):
    seq_count = lax.axis_size("seq")
    bat_count = lax.axis_size("bat")
    seq_index = lax.axis_index("seq")
    bat_index = lax.axis_index("bat")
    batch_rows, local_length, channels = tokens.shape
    rows_local = N1 // seq_count
    spread = channels % (seq_count * bat_count) == 0
    if spread:
        axes, groups = ("bat", "seq"), bat_count
        own = channels // (seq_count * bat_count)
        first = (bat_index * seq_count + seq_index) * own
        sequences = batch_rows * bat_count
    else:
        axes, groups = ("seq",), 1
        own = channels // seq_count
        first = seq_index * own
        sequences = batch_rows
        filter_spectrum = lax.all_gather(filter_spectrum, "bat", axis=3, tiled=True)
    ranks = seq_count * groups

    laid = tokens.reshape(batch_rows, rows_local, N2, channels).transpose(3, 0, 1, 2)
    laid = laid.reshape(ranks, own, batch_rows, rows_local, N2)
    columns = lax.all_to_all(laid, axes, split_axis=0, concat_axis=0, tiled=True)
    columns = columns.reshape(groups, seq_count, own, batch_rows, rows_local, N2)
    if batch_rows == 1:
        columns = columns.reshape(sequences, seq_count, own, rows_local, N2)
    else:
        columns = columns.transpose(0, 3, 1, 2, 4, 5).reshape(sequences, seq_count, own, rows_local, N2)

    spread_filters = filter_spectrum.transpose(3, 0, 1, 2).reshape(seq_count, own, 2, rows_local, N2)
    filters = lax.all_to_all(spread_filters, "seq", split_axis=0, concat_axis=0, tiled=True)
    gain = lax.dynamic_slice(skip_gain, (first,), (own,))
    tables = dft_tables(jnp.arange(N1, dtype=jnp.int32))
    aligned = rows_local % 16 == 0
    if not aligned:
        columns = columns.transpose(0, 2, 1, 3, 4).reshape(sequences, 1, own, N1, N2)
        filters = filters.transpose(1, 2, 0, 3, 4).reshape(1, own, 2, N1, N2)
    chunks = 2 if own % 2 == 0 else 1
    count = own // chunks
    results = []
    for chunk in range(chunks):
        result = convolve(columns, filters, gain, tables, chunk * count, count)
        if not aligned:
            result = result.reshape(sequences, count, seq_count, rows_local, N2).transpose(0, 2, 1, 3, 4)
        if batch_rows == 1:
            result = result.reshape(ranks, count, 1, rows_local, N2)
        else:
            result = result.reshape(groups, batch_rows, seq_count, count, rows_local, N2)
            result = result.transpose(0, 2, 3, 1, 4, 5).reshape(ranks, count, batch_rows, rows_local, N2)
        results.append(lax.all_to_all(result, axes, split_axis=0, concat_axis=0, tiled=True))
    restored = jnp.concatenate(results, axis=1).reshape(channels, batch_rows, rows_local, N2)
    return restored.transpose(1, 2, 3, 0).reshape(batch_rows, local_length, channels)


def relative_rows(index, count, held):
    half = count // 2
    near = index // half * half + jnp.arange(half, dtype=jnp.int32)
    far = index ^ (half + jnp.arange(half, dtype=jnp.int32))
    pieces = jnp.concatenate([near, far])
    return (pieces[:, None] * held + jnp.arange(held, dtype=jnp.int32)[None, :]).reshape(-1)


PAD = 8
LANES = 4


def blocks_of(half, place, kept, far):
    index, base = place[0], place[1]
    near = [(base + block, kept.at[block]) for block in range(half)]
    return near + [(index ^ (half + step), ref) for step, ref in enumerate(far)]


def put_rows(scratch, at, turned):
    for side in range(2):
        scratch[side, at] = turned[:, side * 128 : side * 128 + 128]


def send_rows(scratch, start, stride, message, slot):
    rows = message.shape[1]
    for side in range(2):
        piece = scratch[side, pl.ds(start, rows, stride=stride)]
        message[slot, :, side * 128 : side * 128 + 128] = piece.astype(jnp.bfloat16)


def pack_tokens_kernel(half, groups, place, tokens, kept, *rest):
    far, scratch = rest[:half], rest[half]
    step = pl.program_id(0)
    rows, _, channels = tokens.shape
    stride = channels + PAD
    own = channels // (groups * 2 * half)
    for row in range(rows):
        at = pl.ds(pl.multiple_of((step * rows + row) * stride, PAD), channels)
        put_rows(scratch, at, tokens[row].T.astype(jnp.float32))

    @pl.when(step == pl.num_programs(0) - 1)
    def _():
        for target, message in blocks_of(half, place, kept, far):

            def fill(lane, _):
                for group in range(groups):
                    start = group * (channels // groups) + target * own + lane
                    send_rows(scratch, start, stride, message, group * own + lane)
                return 0

            lax.fori_loop(0, own, fill, 0, unroll=2)


def pack_filters_kernel(half, place, filters, kept, *rest):
    far, scratch = rest[:half], rest[half]
    step = pl.program_id(0)
    _, rows, _, held = filters.shape
    stride = held + PAD
    total = rows * pl.num_programs(0)
    own = held // (2 * half)
    for part in range(2):
        for row in range(rows):
            at = pl.ds(pl.multiple_of((part * total + step * rows + row) * stride, PAD), held)
            put_rows(scratch, at, filters[part, row].T.astype(jnp.float32))

    @pl.when(step == pl.num_programs(0) - 1)
    def _():
        for target, message in blocks_of(half, place, kept, far):

            def fill(lane, _):
                for part in range(2):
                    start = part * total * stride + target * own + lane
                    send_rows(scratch, start, stride, message, 2 * lane + part)
                return 0

            lax.fori_loop(0, own, fill, 0, unroll=2)


VMEM = pl.BlockSpec(memory_space=pltpu.VMEM)
SMEM = pl.BlockSpec(memory_space=pltpu.SMEM)


def message_shapes(half, slots, rows):
    message = jax.ShapeDtypeStruct((slots, rows, N2), jnp.bfloat16)
    return [jax.ShapeDtypeStruct((half, slots, rows, N2), jnp.bfloat16)] + [message] * half


def pack_tokens(place, tokens, half, groups):
    rows, _, channels = tokens.shape
    steps = 2
    return pl.pallas_call(
        functools.partial(pack_tokens_kernel, half, groups),
        grid=(steps,),
        in_specs=[SMEM, pl.BlockSpec((rows // steps, N2, channels), lambda s: (s, 0, 0))],
        out_specs=[VMEM] * (half + 1),
        out_shape=message_shapes(half, channels // (2 * half), rows),
        scratch_shapes=[pltpu.VMEM((2, rows * (channels + PAD), 128), jnp.float32)],
        name="pack_tokens",
    )(place, tokens)


def pack_filters(place, filters, half):
    _, rows, _, held = filters.shape
    steps = 2
    return pl.pallas_call(
        functools.partial(pack_filters_kernel, half),
        grid=(steps,),
        in_specs=[SMEM, pl.BlockSpec((2, rows // steps, N2, held), lambda s: (0, s, 0, 0))],
        out_specs=[VMEM] * (half + 1),
        out_shape=message_shapes(half, held // half, rows),
        scratch_shapes=[pltpu.VMEM((2, 2 * rows * (held + PAD), 128), jnp.float32)],
        name="pack_filters",
    )(place, filters)


def gather_kernel(*refs):
    *far, out = refs
    for step, block in enumerate(far):
        out[step] = block[...]


def gather(far):
    return pl.pallas_call(
        gather_kernel,
        in_specs=[VMEM] * len(far),
        out_specs=VMEM,
        out_shape=jax.ShapeDtypeStruct((len(far), *far[0].shape), jnp.bfloat16),
        name="gather",
    )(*far)


def take(kept, far, slot):
    near = kept[:, pl.ds(slot, 1)].reshape(N1 // 2, N2)
    if not isinstance(far, (list, tuple)):
        return near, far[:, pl.ds(slot, 1)].reshape(N1 // 2, N2)
    across = [ref[pl.ds(slot, 1)].reshape(ref.shape[1], N2) for ref in far]
    return near, jnp.concatenate(across, axis=0)


def forward_kernel(half, lanes, kept, *rest):
    far = rest[:half]
    rows_t, twiddle, cols_t, spectrum = rest[half:]
    slots = [pl.program_id(0) * lanes + lane for lane in range(lanes)]
    turned = []
    for slot in slots:
        signal = jnp.concatenate(take(kept, far, slot), axis=0)
        section = dot(rows_t[...].reshape(2 * N1, N1), signal)
        real, imag = section[:N1], section[N1:]
        turned_real = (real * twiddle[0] + imag * twiddle[1]).astype(jnp.bfloat16)
        turned_imag = (imag * twiddle[0] - real * twiddle[1]).astype(jnp.bfloat16)
        turned.append(jnp.concatenate([turned_real, turned_imag], axis=1))
    result = dot(jnp.concatenate(turned, axis=0), cols_t[...].reshape(2 * N2, 2 * N2))
    for lane, slot in enumerate(slots):
        spectrum[slot] = result[lane * N1 : (lane + 1) * N1].astype(jnp.bfloat16)


def forward(messages, rows_t, twiddle, cols_t):
    kept, *far = messages
    half, slots = kept.shape[:2]
    return pl.pallas_call(
        functools.partial(forward_kernel, half, LANES),
        grid=(slots // LANES,),
        in_specs=[VMEM] * (half + 4),
        out_specs=VMEM,
        out_shape=jax.ShapeDtypeStruct((slots, N1, 2 * N2), jnp.bfloat16),
        name="forward",
    )(kept, *far, rows_t, twiddle, cols_t)


def inverse_kernel(half, own, other, whole, parts, lanes, place, gain, kept, *rest):
    far = rest[:half]
    spectrum, twiddle, back_t, final_t, near_filter = rest[half : half + 5]
    far_filter = rest[half + 5 : half + 5 + parts]
    if parts == 1:
        far_filter = far_filter[0]
    outs = rest[half + 5 + parts :]
    index, base, core = place[0], place[1], place[2]
    piece = kept.shape[2]
    group = core ^ other
    products = []
    lanes_all = [pl.program_id(0) * lanes + number for number in range(lanes)]
    for lane in lanes_all:
        slot = group * own + lane
        weight_real = jnp.concatenate(take(near_filter, far_filter, 2 * lane), axis=0).astype(jnp.float32)
        weight_imag = jnp.concatenate(take(near_filter, far_filter, 2 * lane + 1), axis=0).astype(jnp.float32)
        spec_real = spectrum[slot, :, :N2].astype(jnp.float32)
        spec_imag = spectrum[slot, :, N2:].astype(jnp.float32)
        prod_real = (spec_real * weight_real - spec_imag * weight_imag).astype(jnp.bfloat16)
        prod_imag = (spec_real * weight_imag + spec_imag * weight_real).astype(jnp.bfloat16)
        products.append(jnp.concatenate([prod_real, prod_imag], axis=1))
    back = dot(jnp.concatenate(products, axis=0), back_t[...].reshape(2 * N2, 2 * N2))
    for number, lane in enumerate(lanes_all):
        back_real = back[number * N1 : (number + 1) * N1, :N2]
        back_imag = back[number * N1 : (number + 1) * N1, N2:]
        turned_real = (back_real * twiddle[0] - back_imag * twiddle[1]).astype(jnp.bfloat16)
        turned_imag = (back_real * twiddle[1] + back_imag * twiddle[0]).astype(jnp.bfloat16)
        filtered = dot(final_t[...], jnp.concatenate([turned_real, turned_imag], axis=0))
        slot = group * own + lane
        weight = gain[(group * 2 * half + index) * own + lane]
        direct = jnp.concatenate(take(kept, far, slot), axis=0).astype(jnp.float32)
        result = (filtered + weight * direct).astype(jnp.bfloat16)
        near = pl.ds(base, half) if whole else pl.ds(0, half)
        outs[0][near, pl.ds(lane, 1)] = result[: N1 // 2].reshape(half, 1, piece, N2)
        for step in range(half):
            start = N1 // 2 + step * piece
            rows = result[start : start + piece].reshape(1, piece, N2)
            if whole:
                outs[0][index ^ (half + step), pl.ds(lane, 1)] = rows
            else:
                outs[1 + step][pl.ds(lane, 1)] = rows


def inverse(place, gain, messages, spectrum, tables, filters, own, other, whole):
    kept, *far = messages
    half, _, rows, _ = kept.shape
    if whole:
        out_shape = [jax.ShapeDtypeStruct((2 * half, own, rows, N2), jnp.bfloat16)]
    else:
        out_shape = message_shapes(half, own, rows)
    inputs = [kept, *far, spectrum, *tables, *filters]
    return pl.pallas_call(
        functools.partial(inverse_kernel, half, own, other, whole, len(filters) - 1, LANES),
        grid=(own // LANES,),
        in_specs=[SMEM, SMEM] + [VMEM] * len(inputs),
        out_specs=[VMEM] * len(out_shape),
        out_shape=out_shape,
    )(place, gain, *inputs)


def unpack_kernel(half, whole, place, *rest):
    inputs, out, scratch = rest[: 1 if whole else half + 1], rest[-2], rest[-1]
    step = pl.program_id(0)
    rows, _, held = out.shape
    stride = held + PAD
    total = rows * pl.num_programs(0)

    @pl.when(step == 0)
    def _():
        own = held // (2 * half)
        if whole:
            blocks = [(block, inputs[0].at[block]) for block in range(2 * half)]
        else:
            blocks = blocks_of(half, place, inputs[0], inputs[1:])
        for source, message in blocks:

            def place_rows(lane, _):
                piece = message[lane].astype(jnp.float32)
                put_rows(scratch, pl.ds(source * own + lane, total, stride=stride), piece)
                return 0

            lax.fori_loop(0, own, place_rows, 0, unroll=2)

    for row in range(rows):
        at = pl.ds(pl.multiple_of((step * rows + row) * stride, PAD), held)
        block = jnp.concatenate([scratch[0, at], scratch[1, at]], axis=1)
        out[row] = block.astype(jnp.bfloat16).T


def unpack(place, received, rows, channels, groups, half, other, partial):
    whole = len(received) == 1
    held = channels // groups
    steps = 2
    inputs = [*received, *partial]
    return pl.pallas_call(
        functools.partial(unpack_kernel, half, whole),
        grid_spec=pltpu.PrefetchScalarGridSpec(
            num_scalar_prefetch=1,
            grid=(steps,),
            in_specs=[VMEM] * len(received) + [pl.BlockSpec(memory_space=pl.ANY)] * len(partial),
            out_specs=pl.BlockSpec((rows // steps, N2, held), lambda s, place: (s, 0, place[2] ^ other)),
            scratch_shapes=[pltpu.VMEM((2, rows * (held + PAD), 128), jnp.float32)],
        ),
        out_shape=jax.ShapeDtypeStruct((rows, N2, channels), jnp.bfloat16),
        input_output_aliases={1 + len(received): 0} if partial else {},
    )(place, *inputs)


def exchange(messages, count):
    kept, *far = messages
    half = count // 2
    halves = [list(range(half)), list(range(half, count))]
    across = [
        lax.ppermute(block, "seq", [(s, s ^ (half + step)) for s in range(count)])
        for step, block in enumerate(far)
    ]
    near = lax.all_to_all(kept, "seq", split_axis=0, concat_axis=0, tiled=True, axis_index_groups=halves)
    return [near, *across]


def swap(array):
    return lax.ppermute(array, "bat", [(0, 1), (1, 0)])


def direct_body(tokens, filter_spectrum, skip_gain):
    count = lax.axis_size("seq")
    groups = lax.axis_size("bat")
    index = lax.axis_index("seq")
    core = lax.axis_index("bat")
    _, local_length, channels = tokens.shape
    rows = N1 // count
    half = count // 2
    own = channels // (groups * count)
    place = jnp.stack([index, index // half * half, core]).astype(jnp.int32)
    messages = pack_tokens(place, tokens.reshape(rows, N2, channels), half, groups)
    signal = exchange(messages, count)
    messages = pack_filters(place, filter_spectrum, half)
    filters = exchange(messages, count)
    rows_t, twiddle, cols_t, back_t, final_t = dft_tables(relative_rows(index, count, rows))
    spectrum = forward(signal, rows_t, twiddle, cols_t)
    tables = (twiddle, back_t, jnp.concatenate([final_t[0], final_t[1]], axis=1))
    (ready,) = inverse(place, skip_gain, signal, spectrum, tables, filters, own, 0, True)
    first = lax.all_to_all(ready, "seq", split_axis=0, concat_axis=0, tiled=True)
    near_filter = swap(filters[0])
    far_filter = gather(filters[1:])
    far_filter = swap(far_filter)
    messages = inverse(
        place, skip_gain, signal, spectrum, tables, (near_filter, far_filter), own, 1, False
    )
    second = exchange(messages, count)
    mixed = unpack(place, [first], rows, channels, groups, half, 0, [])
    mixed = unpack(place, second, rows, channels, groups, half, 1, [mixed])
    return mixed.reshape(1, local_length, channels)


def direct_fits(tokens, count, groups):
    batch_rows, _, channels = tokens.shape
    power = count > 2 and count & (count - 1) == 0
    return power and groups == 2 and batch_rows == 1 and N1 // count % 16 == 0 and channels // groups % (LANES * count) == 0


def body(tokens, filter_spectrum, skip_gain):
    if direct_fits(tokens, lax.axis_size("seq"), lax.axis_size("bat")):
        return direct_body(tokens, filter_spectrum, skip_gain)
    return spread_body(tokens, filter_spectrum, skip_gain)


def solution(mesh):
    placed = (P("bat", "seq", None), P(None, "seq", None, "bat"), P())
    return jax.shard_map(
        body, mesh=mesh, in_specs=placed, out_specs=P("bat", "seq", None), check_vma=False
    )
```

```python
import functools
import math

import jax
import jax.numpy as jnp
from jax import lax
from jax.experimental import pallas as pl
from jax.experimental.pallas import tpu as pltpu
from jax.sharding import PartitionSpec as P


N1 = 256
N2 = 256


def cos_sin(points):
    steps_range = jnp.arange(points, dtype=jnp.int32)
    index_grid = steps_range[:, None] * steps_range[None, :] % points
    phase_angle = index_grid.astype(jnp.float32) * (2.0 * math.pi / points)
    return (jnp.cos(phase_angle), jnp.sin(phase_angle))


def dft_tables(order):
    index_grid = order[:, None] * order[None, :] % N1
    phase_angle = index_grid.astype(jnp.float32) * (2.0 * math.pi / N1)
    cos1, sin1 = jnp.cos(phase_angle), jnp.sin(phase_angle)
    cos2, sin2 = cos_sin(N2)
    forward_rows = jnp.stack([cos1, -sin1]).astype(jnp.bfloat16)
    top = jnp.concatenate([cos2, -sin2], axis=1)
    low = jnp.concatenate([sin2, cos2], axis=1)
    forward_cols = jnp.stack([top, low]).astype(jnp.bfloat16)
    top = jnp.concatenate([cos2, sin2], axis=1)
    low = jnp.concatenate([-sin2, cos2], axis=1)
    inverse_cols = (jnp.stack([top, low]) / N2).astype(jnp.bfloat16)
    inverse_rows = (jnp.stack([cos1, -sin1]) / N1).astype(jnp.bfloat16)
    period = N1 * N2
    cols = jnp.arange(N2, dtype=jnp.int32)
    angle = (order[:, None] * cols[None, :] % period).astype(jnp.float32) * (2.0 * math.pi / period)
    twiddle = jnp.stack([jnp.cos(angle), jnp.sin(angle)])
    return forward_rows, twiddle, forward_cols, inverse_cols, inverse_rows


def dot(left, right):
    return jnp.dot(left, right, preferred_element_type=jnp.float32)


def span(block, step, held):
    if held <= step:
        return pl.ds(block * step // held, step // held), pl.ds(0, held)
    return pl.ds(block * step // held, 1), pl.ds(block * step % held, step)


def convolve_kernel(blocks, gain, tokens, filters, rows_t, twiddle, cols_t, back_t, final_t, out, turned_back):
    signal = tokens[0, :, 0].reshape(N1, N2)
    step = N1 // blocks
    for block in range(blocks):
        rows = pl.ds(block * step, step)
        real = dot(rows_t[0, rows], signal)
        imag = dot(rows_t[1, rows], signal)
        cosine = twiddle[0, rows]
        sine = twiddle[1, rows]
        turned_real = (real * cosine + imag * sine).astype(jnp.bfloat16)
        turned_imag = (imag * cosine - real * sine).astype(jnp.bfloat16)
        spectrum = dot(turned_real, cols_t[0]) + dot(turned_imag, cols_t[1])
        spectrum = spectrum.astype(jnp.bfloat16).astype(jnp.float32)
        parts, inner = span(block, step, filters.shape[3])
        weight_real = filters[parts, 0, 0, inner].reshape(step, N2).astype(jnp.float32)
        weight_imag = filters[parts, 0, 1, inner].reshape(step, N2).astype(jnp.float32)
        spec_real, spec_imag = spectrum[:, :N2], spectrum[:, N2:]
        prod_real = (spec_real * weight_real - spec_imag * weight_imag).astype(jnp.bfloat16)
        prod_imag = (spec_real * weight_imag + spec_imag * weight_real).astype(jnp.bfloat16)
        back = dot(prod_real, back_t[0]) + dot(prod_imag, back_t[1])
        back_real, back_imag = back[:, :N2], back[:, N2:]
        turned_back[0, rows] = (back_real * cosine - back_imag * sine).astype(jnp.bfloat16)
        turned_back[1, rows] = (back_real * sine + back_imag * cosine).astype(jnp.bfloat16)
    weight = gain[pl.program_id(0)]
    for block in range(blocks):
        rows = pl.ds(block * step, step)
        parts, inner = span(block, step, tokens.shape[3])
        filtered = dot(final_t[0, rows], turned_back[0]) + dot(final_t[1, rows], turned_back[1])
        direct = tokens[0, parts, 0, inner].reshape(step, N2).astype(jnp.float32)
        result = (filtered + weight * direct).astype(jnp.bfloat16)
        out[0, parts, 0, inner] = result.reshape(parts.size, inner.size, N2)


def convolve(tokens, filters, gain, tables, start, count):
    batch, pieces, _, rows, _ = tokens.shape
    blocks = 2

    def whole(array):
        return pl.BlockSpec(array.shape, lambda c, b: (0,) * array.ndim)

    block = (1, pieces, 1, rows, N2)
    return pl.pallas_call(
        functools.partial(convolve_kernel, blocks),
        grid=(count, batch),
        in_specs=[
            pl.BlockSpec(memory_space=pltpu.SMEM),
            pl.BlockSpec(block, lambda c, b: (b, 0, c + start, 0, 0)),
            pl.BlockSpec((pieces, 1, 2, rows, N2), lambda c, b: (0, c + start, 0, 0, 0)),
            *[whole(table) for table in tables],
        ],
        out_specs=pl.BlockSpec(block, lambda c, b: (b, 0, c, 0, 0)),
        out_shape=jax.ShapeDtypeStruct((batch, pieces, count, rows, N2), jnp.bfloat16),
        scratch_shapes=[pltpu.VMEM((2, N1, N2), jnp.bfloat16)],
        name="convolve",
    )(gain[start : start + count], tokens, filters, *tables)


def spread_body(tokens, filter_spectrum, skip_gain):
    seq_count = lax.axis_size("seq")
    bat_count = lax.axis_size("bat")
    seq_index = lax.axis_index("seq")
    bat_index = lax.axis_index("bat")
    batch_rows, local_length, channels = tokens.shape
    rows_local = N1 // seq_count
    spread = channels % (seq_count * bat_count) == 0
    if spread:
        axes, groups = ("bat", "seq"), bat_count
        own = channels // (seq_count * bat_count)
        first = (bat_index * seq_count + seq_index) * own
        sequences = batch_rows * bat_count
    else:
        axes, groups = ("seq",), 1
        own = channels // seq_count
        first = seq_index * own
        sequences = batch_rows
        filter_spectrum = lax.all_gather(filter_spectrum, "bat", axis=3, tiled=True)
    ranks = seq_count * groups

    laid = tokens.reshape(batch_rows, rows_local, N2, channels).transpose(3, 0, 1, 2)
    laid = laid.reshape(ranks, own, batch_rows, rows_local, N2)
    columns = lax.all_to_all(laid, axes, split_axis=0, concat_axis=0, tiled=True)
    columns = columns.reshape(groups, seq_count, own, batch_rows, rows_local, N2)
    if batch_rows == 1:
        columns = columns.reshape(sequences, seq_count, own, rows_local, N2)
    else:
        columns = columns.transpose(0, 3, 1, 2, 4, 5).reshape(sequences, seq_count, own, rows_local, N2)

    spread_filters = filter_spectrum.transpose(3, 0, 1, 2).reshape(seq_count, own, 2, rows_local, N2)
    filters = lax.all_to_all(spread_filters, "seq", split_axis=0, concat_axis=0, tiled=True)
    gain = lax.dynamic_slice(skip_gain, (first,), (own,))
    tables = dft_tables(jnp.arange(N1, dtype=jnp.int32))
    aligned = rows_local % 16 == 0
    if not aligned:
        columns = columns.transpose(0, 2, 1, 3, 4).reshape(sequences, 1, own, N1, N2)
        filters = filters.transpose(1, 2, 0, 3, 4).reshape(1, own, 2, N1, N2)
    chunks = 2 if own % 2 == 0 else 1
    count = own // chunks
    results = []
    for chunk in range(chunks):
        result = convolve(columns, filters, gain, tables, chunk * count, count)
        if not aligned:
            result = result.reshape(sequences, count, seq_count, rows_local, N2).transpose(0, 2, 1, 3, 4)
        if batch_rows == 1:
            result = result.reshape(ranks, count, 1, rows_local, N2)
        else:
            result = result.reshape(groups, batch_rows, seq_count, count, rows_local, N2)
            result = result.transpose(0, 2, 3, 1, 4, 5).reshape(ranks, count, batch_rows, rows_local, N2)
        results.append(lax.all_to_all(result, axes, split_axis=0, concat_axis=0, tiled=True))
    restored = jnp.concatenate(results, axis=1).reshape(channels, batch_rows, rows_local, N2)
    return restored.transpose(1, 2, 3, 0).reshape(batch_rows, local_length, channels)


def relative_rows(index, count, held):
    half = count // 2
    near = index // half * half + jnp.arange(half, dtype=jnp.int32)
    far = index ^ (half + jnp.arange(half, dtype=jnp.int32))
    pieces = jnp.concatenate([near, far])
    return (pieces[:, None] * held + jnp.arange(held, dtype=jnp.int32)[None, :]).reshape(-1)


PAD = 8
LANES = 4
TRANSFORM_MIB = 32


def blocks_of(half, place, kept, far):
    index, base = place[0], place[1]
    near = [(base + block, kept.at[block]) for block in range(half)]
    return near + [(index ^ (half + step), ref) for step, ref in enumerate(far)]


def put_rows(scratch, at, turned):
    for side in range(2):
        scratch[side, at] = turned[:, side * 128 : side * 128 + 128]


def send_rows(scratch, start, stride, message, slot):
    rows = message.shape[1]
    for side in range(2):
        piece = scratch[side, pl.ds(start, rows, stride=stride)]
        message[slot, :, side * 128 : side * 128 + 128] = piece.astype(jnp.bfloat16)


def pack_tokens_kernel(half, place, tokens, *rest):
    kept, *far, scratch = rest
    step = pl.program_id(0)
    rows, _, held = tokens.shape
    stride = held + PAD
    own = held // (2 * half)
    for row in range(rows):
        at = pl.ds(pl.multiple_of((step * rows + row) * stride, PAD), held)
        put_rows(scratch, at, tokens[row].T.astype(jnp.float32))

    @pl.when(step == pl.num_programs(0) - 1)
    def _():
        for target, message in blocks_of(half, place, kept, far):

            def fill(lane, _):
                send_rows(scratch, target * own + lane, stride, message, lane)
                return 0

            lax.fori_loop(0, own, fill, 0, unroll=4)


def pack_filters_kernel(half, place, filters, before, kept, *rest):
    far, scratch = rest[:half], rest[half]
    step = pl.program_id(0)
    _, rows, _, held = filters.shape
    stride = held + PAD
    total = rows * pl.num_programs(0)
    own = held // (2 * half)
    for part in range(2):
        for row in range(rows):
            at = pl.ds(pl.multiple_of((part * total + step * rows + row) * stride, PAD), held)
            put_rows(scratch, at, filters[part, row].T.astype(jnp.float32))

    @pl.when(step == pl.num_programs(0) - 1)
    def _():
        kept[:, :own] = before[...]
        for number, (target, message) in enumerate(blocks_of(half, place, kept, far)):
            first = own if number < half else 0

            def fill(lane, _):
                for part in range(2):
                    start = part * total * stride + target * own + lane
                    send_rows(scratch, start, stride, message, first + 2 * lane + part)
                return 0

            lax.fori_loop(0, own, fill, 0, unroll=2)


VMEM = pl.BlockSpec(memory_space=pltpu.VMEM)
SMEM = pl.BlockSpec(memory_space=pltpu.SMEM)


def message_shapes(half, slots, rows):
    message = jax.ShapeDtypeStruct((slots, rows, N2), jnp.bfloat16)
    return [jax.ShapeDtypeStruct((half, slots, rows, N2), jnp.bfloat16)] + [message] * half


def pack_tokens(place, tokens, half, groups, other):
    rows, _, channels = tokens.shape
    held = channels // groups
    own = held // (2 * half)
    steps = 2
    block = pl.BlockSpec((rows // steps, N2, held), lambda s, place: (s, 0, place[2] ^ other))
    return pl.pallas_call(
        functools.partial(pack_tokens_kernel, half),
        grid_spec=pltpu.PrefetchScalarGridSpec(
            num_scalar_prefetch=1,
            grid=(steps,),
            in_specs=[block],
            out_specs=[VMEM] * (half + 1),
            scratch_shapes=[pltpu.VMEM((2, rows * (held + PAD), 128), jnp.float32)],
        ),
        out_shape=message_shapes(half, own, rows),
    )(place, tokens)


def pack_filters(place, filters, before, half):
    _, rows, _, held = filters.shape
    steps = 2
    kept = jax.ShapeDtypeStruct((half, before.shape[1] + held // half, rows, N2), jnp.bfloat16)
    return pl.pallas_call(
        functools.partial(pack_filters_kernel, half),
        grid=(steps,),
        in_specs=[SMEM, pl.BlockSpec((2, rows // steps, N2, held), lambda s: (0, s, 0, 0)), VMEM],
        out_specs=[VMEM] * (half + 1),
        out_shape=[kept] + message_shapes(half, held // half, rows)[1:],
        scratch_shapes=[pltpu.VMEM((2, 2 * rows * (held + PAD), 128), jnp.float32)],
        name="pack_filters",
    )(place, filters, before)


def gather_kernel(*refs):
    *far, out = refs
    for step, block in enumerate(far):
        out[step] = block[...]


def gather(far):
    return pl.pallas_call(
        gather_kernel,
        in_specs=[VMEM] * len(far),
        out_specs=VMEM,
        out_shape=jax.ShapeDtypeStruct((len(far), *far[0].shape), jnp.bfloat16),
        compiler_params=pltpu.CompilerParams(vmem_limit_bytes=8 * 1024 * 1024),
        name="gather",
    )(*far)


def take(near, far, near_slot, far_slot):
    if not isinstance(far, (list, tuple)):
        across = [far[:, pl.ds(far_slot, 1)].reshape(N1 // 2, N2)]
    else:
        across = [ref[pl.ds(far_slot, 1)].reshape(ref.shape[1], N2) for ref in far]
    return jnp.concatenate([near[:, pl.ds(near_slot, 1)].reshape(N1 // 2, N2), *across], axis=0)


def transform_kernel(half, own, other, whole, parts, lanes, place, gain, kept, *rest):
    far = rest[:half]
    rows_t, twiddle, cols_t, back_t, final_t = rest[half : half + 5]
    filters, outs = rest[half + 5 : half + 5 + parts], rest[half + 5 + parts :]
    near_filter, far_filter = (kept, filters) if parts == half else filters
    index, base, core = place[0], place[1], place[2]
    piece = kept.shape[2]
    channels = [pl.program_id(0) * lanes + number for number in range(lanes)]

    turned = []
    for lane in channels:
        section = dot(rows_t[...].reshape(2 * N1, N1), take(kept, far, lane, lane))
        real, imag = section[:N1], section[N1:]
        turned_real = (real * twiddle[0] + imag * twiddle[1]).astype(jnp.bfloat16)
        turned_imag = (imag * twiddle[0] - real * twiddle[1]).astype(jnp.bfloat16)
        turned.append(jnp.concatenate([turned_real, turned_imag], axis=1))
    spectrum = dot(jnp.concatenate(turned, axis=0), cols_t[...].reshape(2 * N2, 2 * N2))
    spectrum = spectrum.astype(jnp.bfloat16)
    products = []
    for number, lane in enumerate(channels):
        real, imag = 2 * lane, 2 * lane + 1
        weight_real = take(near_filter, far_filter, own + real, real).astype(jnp.float32)
        weight_imag = take(near_filter, far_filter, own + imag, imag).astype(jnp.float32)
        spec_real = spectrum[number * N1 : (number + 1) * N1, :N2].astype(jnp.float32)
        spec_imag = spectrum[number * N1 : (number + 1) * N1, N2:].astype(jnp.float32)
        prod_real = (spec_real * weight_real - spec_imag * weight_imag).astype(jnp.bfloat16)
        prod_imag = (spec_real * weight_imag + spec_imag * weight_real).astype(jnp.bfloat16)
        products.append(jnp.concatenate([prod_real, prod_imag], axis=1))
    back = dot(jnp.concatenate(products, axis=0), back_t[...].reshape(2 * N2, 2 * N2))
    for number, lane in enumerate(channels):
        back_real = back[number * N1 : (number + 1) * N1, :N2]
        back_imag = back[number * N1 : (number + 1) * N1, N2:]
        turned_real = (back_real * twiddle[0] - back_imag * twiddle[1]).astype(jnp.bfloat16)
        turned_imag = (back_real * twiddle[1] + back_imag * twiddle[0]).astype(jnp.bfloat16)
        filtered = dot(final_t[...], jnp.concatenate([turned_real, turned_imag], axis=0))
        weight = gain[((core ^ other) * 2 * half + index) * own + lane]
        result = (filtered + weight * take(kept, far, lane, lane).astype(jnp.float32)).astype(jnp.bfloat16)
        near = pl.ds(base, half) if whole else pl.ds(0, half)
        outs[0][near, pl.ds(lane, 1)] = result[: N1 // 2].reshape(half, 1, piece, N2)
        for step in range(half):
            start = N1 // 2 + step * piece
            rows = result[start : start + piece].reshape(1, piece, N2)
            if whole:
                outs[0][index ^ (half + step), pl.ds(lane, 1)] = rows
            else:
                outs[1 + step][pl.ds(lane, 1)] = rows


def transform(place, gain, kept, far, tables, filters, other, whole):
    half, _, rows, _ = kept.shape
    own = far[0].shape[0]
    if whole:
        out_shape = [jax.ShapeDtypeStruct((2 * half, own, rows, N2), jnp.bfloat16)]
    else:
        out_shape = message_shapes(half, own, rows)
    inputs = [kept, *far, *tables, *filters]
    return pl.pallas_call(
        functools.partial(transform_kernel, half, own, other, whole, len(filters), LANES),
        grid=(own // LANES,),
        in_specs=[SMEM, SMEM] + [VMEM] * len(inputs),
        out_specs=[VMEM] * len(out_shape),
        out_shape=out_shape,
        compiler_params=pltpu.CompilerParams(vmem_limit_bytes=TRANSFORM_MIB * 1024 * 1024),
    )(place, gain, *inputs)


def unpack_kernel(half, whole, place, *rest):
    inputs, out, scratch = rest[: 1 if whole else half + 1], rest[-2], rest[-1]
    step = pl.program_id(0)
    rows, _, held = out.shape
    stride = held + PAD
    total = rows * pl.num_programs(0)

    @pl.when(step == 0)
    def _():
        own = held // (2 * half)
        if whole:
            blocks = [(block, inputs[0].at[block]) for block in range(2 * half)]
        else:
            blocks = blocks_of(half, place, inputs[0], inputs[1:])
        for source, message in blocks:

            def place_rows(lane, _):
                piece = message[lane].astype(jnp.float32)
                put_rows(scratch, pl.ds(source * own + lane, total, stride=stride), piece)
                return 0

            lax.fori_loop(0, own, place_rows, 0, unroll=2)

    for row in range(rows):
        at = pl.ds(pl.multiple_of((step * rows + row) * stride, PAD), held)
        block = jnp.concatenate([scratch[0, at], scratch[1, at]], axis=1)
        out[row] = block.astype(jnp.bfloat16).T


def unpack(place, received, rows, channels, groups, half, other, partial):
    whole = len(received) == 1
    held = channels // groups
    steps = 2
    inputs = [*received, *partial]
    return pl.pallas_call(
        functools.partial(unpack_kernel, half, whole),
        grid_spec=pltpu.PrefetchScalarGridSpec(
            num_scalar_prefetch=1,
            grid=(steps,),
            in_specs=[VMEM] * len(received) + [pl.BlockSpec(memory_space=pl.ANY)] * len(partial),
            out_specs=pl.BlockSpec((rows // steps, N2, held), lambda s, place: (s, 0, place[2] ^ other)),
            scratch_shapes=[pltpu.VMEM((2, rows * (held + PAD), 128), jnp.float32)],
        ),
        out_shape=jax.ShapeDtypeStruct((rows, N2, channels), jnp.bfloat16),
        input_output_aliases={1 + len(received): 0} if partial else {},
        compiler_params=pltpu.CompilerParams(vmem_limit_bytes=12 * 1024 * 1024),
    )(place, *inputs)


def cross(far, count):
    half = count // 2
    return [
        lax.ppermute(block, "seq", [(s, s ^ (half + step)) for s in range(count)])
        for step, block in enumerate(far)
    ]


def near(kept, count):
    half = count // 2
    halves = [list(range(half)), list(range(half, count))]
    return lax.all_to_all(kept, "seq", split_axis=0, concat_axis=0, tiled=True, axis_index_groups=halves)


def swap(array):
    return lax.ppermute(array, "bat", [(0, 1), (1, 0)])


def direct_body(tokens, filter_spectrum, skip_gain):
    count = lax.axis_size("seq")
    groups = lax.axis_size("bat")
    index = lax.axis_index("seq")
    core = lax.axis_index("bat")
    _, local_length, channels = tokens.shape
    rows = N1 // count
    half = count // 2
    place = jnp.stack([index, index // half * half, core]).astype(jnp.int32)
    laid = tokens.reshape(rows, N2, channels)
    kept, *far = pack_tokens(place, laid, half, groups, 0)
    far_own = cross(far, count)
    kept, *far = pack_filters(place, filter_spectrum, kept, half)
    far_filters = cross(far, count)
    kept_own = near(kept, count)
    kept, *far = pack_tokens(place, laid, half, groups, 1)
    far_other = cross(far, count)
    kept_other = near(kept, count)
    *tables, final_t = dft_tables(relative_rows(index, count, rows))
    tables.append(jnp.concatenate([final_t[0], final_t[1]], axis=1))
    (ready,) = transform(place, skip_gain, kept_own, far_own, tables, far_filters, 0, True)
    first = lax.all_to_all(ready, "seq", split_axis=0, concat_axis=0, tiled=True)
    gathered = gather(far_filters)
    filters = (swap(kept_own), swap(gathered))
    kept, *far = transform(place, skip_gain, kept_other, far_other, tables, filters, 1, False)
    far = cross(far, count)
    kept = near(kept, count)
    mixed = unpack(place, [first], rows, channels, groups, half, 0, [])
    mixed = unpack(place, [kept, *far], rows, channels, groups, half, 1, [mixed])
    return mixed.reshape(1, local_length, channels)


def direct_fits(tokens, count, groups):
    batch_rows, _, channels = tokens.shape
    power = count > 2 and count & (count - 1) == 0
    return power and groups == 2 and batch_rows == 1 and N1 // count % 16 == 0 and channels // groups % (LANES * count) == 0


def body(tokens, filter_spectrum, skip_gain):
    if direct_fits(tokens, lax.axis_size("seq"), lax.axis_size("bat")):
        return direct_body(tokens, filter_spectrum, skip_gain)
    return spread_body(tokens, filter_spectrum, skip_gain)


def solution(mesh):
    placed = (P("bat", "seq", None), P(None, "seq", None, "bat"), P())
    return jax.shard_map(
        body, mesh=mesh, in_specs=placed, out_specs=P("bat", "seq", None), check_vma=False
    )
```

```python
import functools
import math

import jax
import jax.numpy as jnp
from jax import lax
from jax.experimental import pallas as pl
from jax.experimental.pallas import tpu as pltpu
from jax.sharding import PartitionSpec as P


N1 = 256
N2 = 256


def cos_sin(points):
    steps_range = jnp.arange(points, dtype=jnp.int32)
    index_grid = steps_range[:, None] * steps_range[None, :] % points
    phase_angle = index_grid.astype(jnp.float32) * (2.0 * math.pi / points)
    return (jnp.cos(phase_angle), jnp.sin(phase_angle))


def dft_tables(order):
    index_grid = order[:, None] * order[None, :] % N1
    phase_angle = index_grid.astype(jnp.float32) * (2.0 * math.pi / N1)
    cos1, sin1 = jnp.cos(phase_angle), jnp.sin(phase_angle)
    cos2, sin2 = cos_sin(N2)
    forward_rows = jnp.stack([cos1, -sin1]).astype(jnp.bfloat16)
    top = jnp.concatenate([cos2, -sin2], axis=1)
    low = jnp.concatenate([sin2, cos2], axis=1)
    forward_cols = jnp.stack([top, low]).astype(jnp.bfloat16)
    top = jnp.concatenate([cos2, sin2], axis=1)
    low = jnp.concatenate([-sin2, cos2], axis=1)
    inverse_cols = (jnp.stack([top, low]) / N2).astype(jnp.bfloat16)
    inverse_rows = (jnp.stack([cos1, -sin1]) / N1).astype(jnp.bfloat16)
    period = N1 * N2
    cols = jnp.arange(N2, dtype=jnp.int32)
    angle = (order[:, None] * cols[None, :] % period).astype(jnp.float32) * (2.0 * math.pi / period)
    twiddle = jnp.stack([jnp.cos(angle), jnp.sin(angle)])
    return forward_rows, twiddle, forward_cols, inverse_cols, inverse_rows


def dot(left, right):
    return jnp.dot(left, right, preferred_element_type=jnp.float32)


def span(block, step, held):
    if held <= step:
        return pl.ds(block * step // held, step // held), pl.ds(0, held)
    return pl.ds(block * step // held, 1), pl.ds(block * step % held, step)


def convolve_kernel(blocks, gain, tokens, filters, rows_t, twiddle, cols_t, back_t, final_t, out, turned_back):
    signal = tokens[0, :, 0].reshape(N1, N2)
    step = N1 // blocks
    for block in range(blocks):
        rows = pl.ds(block * step, step)
        real = dot(rows_t[0, rows], signal)
        imag = dot(rows_t[1, rows], signal)
        cosine = twiddle[0, rows]
        sine = twiddle[1, rows]
        turned_real = (real * cosine + imag * sine).astype(jnp.bfloat16)
        turned_imag = (imag * cosine - real * sine).astype(jnp.bfloat16)
        spectrum = dot(turned_real, cols_t[0]) + dot(turned_imag, cols_t[1])
        spectrum = spectrum.astype(jnp.bfloat16).astype(jnp.float32)
        parts, inner = span(block, step, filters.shape[3])
        weight_real = filters[parts, 0, 0, inner].reshape(step, N2).astype(jnp.float32)
        weight_imag = filters[parts, 0, 1, inner].reshape(step, N2).astype(jnp.float32)
        spec_real, spec_imag = spectrum[:, :N2], spectrum[:, N2:]
        prod_real = (spec_real * weight_real - spec_imag * weight_imag).astype(jnp.bfloat16)
        prod_imag = (spec_real * weight_imag + spec_imag * weight_real).astype(jnp.bfloat16)
        back = dot(prod_real, back_t[0]) + dot(prod_imag, back_t[1])
        back_real, back_imag = back[:, :N2], back[:, N2:]
        turned_back[0, rows] = (back_real * cosine - back_imag * sine).astype(jnp.bfloat16)
        turned_back[1, rows] = (back_real * sine + back_imag * cosine).astype(jnp.bfloat16)
    weight = gain[pl.program_id(0)]
    for block in range(blocks):
        rows = pl.ds(block * step, step)
        parts, inner = span(block, step, tokens.shape[3])
        filtered = dot(final_t[0, rows], turned_back[0]) + dot(final_t[1, rows], turned_back[1])
        direct = tokens[0, parts, 0, inner].reshape(step, N2).astype(jnp.float32)
        result = (filtered + weight * direct).astype(jnp.bfloat16)
        out[0, parts, 0, inner] = result.reshape(parts.size, inner.size, N2)


def convolve(tokens, filters, gain, tables, start, count):
    batch, pieces, _, rows, _ = tokens.shape
    blocks = 2

    def whole(array):
        return pl.BlockSpec(array.shape, lambda c, b: (0,) * array.ndim)

    block = (1, pieces, 1, rows, N2)
    return pl.pallas_call(
        functools.partial(convolve_kernel, blocks),
        grid=(count, batch),
        in_specs=[
            pl.BlockSpec(memory_space=pltpu.SMEM),
            pl.BlockSpec(block, lambda c, b: (b, 0, c + start, 0, 0)),
            pl.BlockSpec((pieces, 1, 2, rows, N2), lambda c, b: (0, c + start, 0, 0, 0)),
            *[whole(table) for table in tables],
        ],
        out_specs=pl.BlockSpec(block, lambda c, b: (b, 0, c, 0, 0)),
        out_shape=jax.ShapeDtypeStruct((batch, pieces, count, rows, N2), jnp.bfloat16),
        scratch_shapes=[pltpu.VMEM((2, N1, N2), jnp.bfloat16)],
        name="convolve",
    )(gain[start : start + count], tokens, filters, *tables)


def spread_body(tokens, filter_spectrum, skip_gain):
    seq_count = lax.axis_size("seq")
    bat_count = lax.axis_size("bat")
    seq_index = lax.axis_index("seq")
    bat_index = lax.axis_index("bat")
    batch_rows, local_length, channels = tokens.shape
    rows_local = N1 // seq_count
    spread = channels % (seq_count * bat_count) == 0
    if spread:
        axes, groups = ("bat", "seq"), bat_count
        own = channels // (seq_count * bat_count)
        first = (bat_index * seq_count + seq_index) * own
        sequences = batch_rows * bat_count
    else:
        axes, groups = ("seq",), 1
        own = channels // seq_count
        first = seq_index * own
        sequences = batch_rows
        filter_spectrum = lax.all_gather(filter_spectrum, "bat", axis=3, tiled=True)
    ranks = seq_count * groups

    laid = tokens.reshape(batch_rows, rows_local, N2, channels).transpose(3, 0, 1, 2)
    laid = laid.reshape(ranks, own, batch_rows, rows_local, N2)
    columns = lax.all_to_all(laid, axes, split_axis=0, concat_axis=0, tiled=True)
    columns = columns.reshape(groups, seq_count, own, batch_rows, rows_local, N2)
    if batch_rows == 1:
        columns = columns.reshape(sequences, seq_count, own, rows_local, N2)
    else:
        columns = columns.transpose(0, 3, 1, 2, 4, 5).reshape(sequences, seq_count, own, rows_local, N2)

    spread_filters = filter_spectrum.transpose(3, 0, 1, 2).reshape(seq_count, own, 2, rows_local, N2)
    filters = lax.all_to_all(spread_filters, "seq", split_axis=0, concat_axis=0, tiled=True)
    gain = lax.dynamic_slice(skip_gain, (first,), (own,))
    tables = dft_tables(jnp.arange(N1, dtype=jnp.int32))
    aligned = rows_local % 16 == 0
    if not aligned:
        columns = columns.transpose(0, 2, 1, 3, 4).reshape(sequences, 1, own, N1, N2)
        filters = filters.transpose(1, 2, 0, 3, 4).reshape(1, own, 2, N1, N2)
    chunks = 2 if own % 2 == 0 else 1
    count = own // chunks
    results = []
    for chunk in range(chunks):
        result = convolve(columns, filters, gain, tables, chunk * count, count)
        if not aligned:
            result = result.reshape(sequences, count, seq_count, rows_local, N2).transpose(0, 2, 1, 3, 4)
        if batch_rows == 1:
            result = result.reshape(ranks, count, 1, rows_local, N2)
        else:
            result = result.reshape(groups, batch_rows, seq_count, count, rows_local, N2)
            result = result.transpose(0, 2, 3, 1, 4, 5).reshape(ranks, count, batch_rows, rows_local, N2)
        results.append(lax.all_to_all(result, axes, split_axis=0, concat_axis=0, tiled=True))
    restored = jnp.concatenate(results, axis=1).reshape(channels, batch_rows, rows_local, N2)
    return restored.transpose(1, 2, 3, 0).reshape(batch_rows, local_length, channels)


def relative_rows(index, count, held):
    half = count // 2
    near = index // half * half + jnp.arange(half, dtype=jnp.int32)
    far = index ^ (half + jnp.arange(half, dtype=jnp.int32))
    pieces = jnp.concatenate([near, far])
    return (pieces[:, None] * held + jnp.arange(held, dtype=jnp.int32)[None, :]).reshape(-1)


PAD = 8
LANES = 4
TRANSFORM_MIB = 32


def blocks_of(half, kept, far):
    index = lax.axis_index("seq")
    base = index // half * half
    near = [(base + block, kept.at[block]) for block in range(half)]
    return near + [(index ^ (half + step), ref) for step, ref in enumerate(far)]


def put_rows(scratch, at, turned):
    for side in range(2):
        scratch[side, at] = turned[:, side * 128 : side * 128 + 128]


def send_rows(scratch, start, stride, message, slot):
    rows = message.shape[1]
    for side in range(2):
        piece = scratch[side, pl.ds(start, rows, stride=stride)]
        message[slot, :, side * 128 : side * 128 + 128] = piece.astype(jnp.bfloat16)


def pack_tokens_kernel(half, tokens, *rest):
    kept, *far, scratch = rest
    step = pl.program_id(0)
    rows, _, held = tokens.shape
    stride = held + PAD
    own = held // (2 * half)
    for row in range(rows):
        at = pl.ds(pl.multiple_of((step * rows + row) * stride, PAD), held)
        put_rows(scratch, at, tokens[row].T.astype(jnp.float32))

    @pl.when(step == pl.num_programs(0) - 1)
    def _():
        for target, message in blocks_of(half, kept, far):

            def fill(lane, _):
                send_rows(scratch, target * own + lane, stride, message, lane)
                return 0

            lax.fori_loop(0, own, fill, 0, unroll=4)


def pack_filters_kernel(half, filters, before, kept, *rest):
    far, scratch = rest[:half], rest[half]
    step = pl.program_id(0)
    _, rows, _, held = filters.shape
    stride = held + PAD
    total = rows * pl.num_programs(0)
    own = held // (2 * half)
    for part in range(2):
        for row in range(rows):
            at = pl.ds(pl.multiple_of((part * total + step * rows + row) * stride, PAD), held)
            put_rows(scratch, at, filters[part, row].T.astype(jnp.float32))

    @pl.when(step == pl.num_programs(0) - 1)
    def _():
        kept[:, :own] = before[...]
        for number, (target, message) in enumerate(blocks_of(half, kept, far)):
            first = own if number < half else 0

            def fill(lane, _):
                for part in range(2):
                    start = part * total * stride + target * own + lane
                    send_rows(scratch, start, stride, message, first + 2 * lane + part)
                return 0

            lax.fori_loop(0, own, fill, 0, unroll=2)


VMEM = pl.BlockSpec(memory_space=pltpu.VMEM)
SMEM = pl.BlockSpec(memory_space=pltpu.SMEM)


def message_shapes(half, slots, rows):
    message = jax.ShapeDtypeStruct((slots, rows, N2), jnp.bfloat16)
    return [jax.ShapeDtypeStruct((half, slots, rows, N2), jnp.bfloat16)] + [message] * half


def pack_tokens(tokens, half, groups, other):
    rows, _, channels = tokens.shape
    held = channels // groups
    own = held // (2 * half)
    steps = 2
    block = pl.BlockSpec((rows // steps, N2, held), lambda s: (s, 0, lax.axis_index("bat") ^ other))
    return pl.pallas_call(
        functools.partial(pack_tokens_kernel, half),
        grid=(steps,),
        in_specs=[block],
        out_specs=[VMEM] * (half + 1),
        scratch_shapes=[pltpu.VMEM((2, rows * (held + PAD), 128), jnp.float32)],
        out_shape=message_shapes(half, own, rows),
    )(tokens)


def pack_filters(filters, before, half):
    _, rows, _, held = filters.shape
    steps = 2
    kept = jax.ShapeDtypeStruct((half, before.shape[1] + held // half, rows, N2), jnp.bfloat16)
    return pl.pallas_call(
        functools.partial(pack_filters_kernel, half),
        grid=(steps,),
        in_specs=[pl.BlockSpec((2, rows // steps, N2, held), lambda s: (0, s, 0, 0)), VMEM],
        out_specs=[VMEM] * (half + 1),
        out_shape=[kept] + message_shapes(half, held // half, rows)[1:],
        scratch_shapes=[pltpu.VMEM((2, 2 * rows * (held + PAD), 128), jnp.float32)],
        name="pack_filters",
    )(filters, before)


def gather_kernel(*refs):
    *far, out = refs
    for step, block in enumerate(far):
        out[step] = block[...]


def gather(far):
    return pl.pallas_call(
        gather_kernel,
        in_specs=[VMEM] * len(far),
        out_specs=VMEM,
        out_shape=jax.ShapeDtypeStruct((len(far), *far[0].shape), jnp.bfloat16),
        compiler_params=pltpu.CompilerParams(vmem_limit_bytes=8 * 1024 * 1024),
        name="gather",
    )(*far)


def take(near, far, near_slot, far_slot):
    if not isinstance(far, (list, tuple)):
        across = [far[:, pl.ds(far_slot, 1)].reshape(N1 // 2, N2)]
    else:
        across = [ref[pl.ds(far_slot, 1)].reshape(ref.shape[1], N2) for ref in far]
    return jnp.concatenate([near[:, pl.ds(near_slot, 1)].reshape(N1 // 2, N2), *across], axis=0)


def transform_kernel(half, own, other, whole, parts, lanes, gain, kept, *rest):
    far = rest[:half]
    rows_t, twiddle, cols_t, back_t, final_t = rest[half : half + 5]
    filters, outs = rest[half + 5 : half + 5 + parts], rest[half + 5 + parts :]
    near_filter, far_filter = (kept, filters) if parts == half else filters
    index, core = lax.axis_index("seq"), lax.axis_index("bat")
    base = index // half * half
    piece = kept.shape[2]
    channels = [pl.program_id(0) * lanes + number for number in range(lanes)]

    turned = []
    for lane in channels:
        section = dot(rows_t[...].reshape(2 * N1, N1), take(kept, far, lane, lane))
        real, imag = section[:N1], section[N1:]
        turned_real = (real * twiddle[0] + imag * twiddle[1]).astype(jnp.bfloat16)
        turned_imag = (imag * twiddle[0] - real * twiddle[1]).astype(jnp.bfloat16)
        turned.append(jnp.concatenate([turned_real, turned_imag], axis=1))
    spectrum = dot(jnp.concatenate(turned, axis=0), cols_t[...].reshape(2 * N2, 2 * N2))
    spectrum = spectrum.astype(jnp.bfloat16)
    products = []
    for number, lane in enumerate(channels):
        real, imag = 2 * lane, 2 * lane + 1
        weight_real = take(near_filter, far_filter, own + real, real).astype(jnp.float32)
        weight_imag = take(near_filter, far_filter, own + imag, imag).astype(jnp.float32)
        spec_real = spectrum[number * N1 : (number + 1) * N1, :N2].astype(jnp.float32)
        spec_imag = spectrum[number * N1 : (number + 1) * N1, N2:].astype(jnp.float32)
        prod_real = (spec_real * weight_real - spec_imag * weight_imag).astype(jnp.bfloat16)
        prod_imag = (spec_real * weight_imag + spec_imag * weight_real).astype(jnp.bfloat16)
        products.append(jnp.concatenate([prod_real, prod_imag], axis=1))
    back = dot(jnp.concatenate(products, axis=0), back_t[...].reshape(2 * N2, 2 * N2))
    for number, lane in enumerate(channels):
        back_real = back[number * N1 : (number + 1) * N1, :N2]
        back_imag = back[number * N1 : (number + 1) * N1, N2:]
        turned_real = (back_real * twiddle[0] - back_imag * twiddle[1]).astype(jnp.bfloat16)
        turned_imag = (back_real * twiddle[1] + back_imag * twiddle[0]).astype(jnp.bfloat16)
        filtered = dot(final_t[...], jnp.concatenate([turned_real, turned_imag], axis=0))
        weight = gain[((core ^ other) * 2 * half + index) * own + lane]
        result = (filtered + weight * take(kept, far, lane, lane).astype(jnp.float32)).astype(jnp.bfloat16)
        near = pl.ds(base, half) if whole else pl.ds(0, half)
        outs[0][near, pl.ds(lane, 1)] = result[: N1 // 2].reshape(half, 1, piece, N2)
        for step in range(half):
            start = N1 // 2 + step * piece
            rows = result[start : start + piece].reshape(1, piece, N2)
            if whole:
                outs[0][index ^ (half + step), pl.ds(lane, 1)] = rows
            else:
                outs[1 + step][pl.ds(lane, 1)] = rows


def transform(gain, kept, far, tables, filters, other, whole):
    half, _, rows, _ = kept.shape
    own = far[0].shape[0]
    if whole:
        out_shape = [jax.ShapeDtypeStruct((2 * half, own, rows, N2), jnp.bfloat16)]
    else:
        out_shape = message_shapes(half, own, rows)
    inputs = [kept, *far, *tables, *filters]
    return pl.pallas_call(
        functools.partial(transform_kernel, half, own, other, whole, len(filters), LANES),
        grid=(own // LANES,),
        in_specs=[SMEM] + [VMEM] * len(inputs),
        out_specs=[VMEM] * len(out_shape),
        out_shape=out_shape,
        compiler_params=pltpu.CompilerParams(vmem_limit_bytes=TRANSFORM_MIB * 1024 * 1024),
    )(gain, *inputs)


def unpack_kernel(half, whole, *rest):
    inputs, out, scratch = rest[: 1 if whole else half + 1], rest[-2], rest[-1]
    step = pl.program_id(0)
    rows, _, held = out.shape
    stride = held + PAD
    total = rows * pl.num_programs(0)

    @pl.when(step == 0)
    def _():
        own = held // (2 * half)
        if whole:
            blocks = [(block, inputs[0].at[block]) for block in range(2 * half)]
        else:
            blocks = blocks_of(half, inputs[0], inputs[1:])
        for source, message in blocks:

            def place_rows(lane, _):
                piece = message[lane].astype(jnp.float32)
                put_rows(scratch, pl.ds(source * own + lane, total, stride=stride), piece)
                return 0

            lax.fori_loop(0, own, place_rows, 0, unroll=2)

    for row in range(rows):
        at = pl.ds(pl.multiple_of((step * rows + row) * stride, PAD), held)
        block = jnp.concatenate([scratch[0, at], scratch[1, at]], axis=1)
        out[row] = block.astype(jnp.bfloat16).T


def unpack(received, rows, channels, groups, half, other, partial):
    whole = len(received) == 1
    held = channels // groups
    steps = 2
    inputs = [*received, *partial]
    return pl.pallas_call(
        functools.partial(unpack_kernel, half, whole),
        grid=(steps,),
        in_specs=[VMEM] * len(received) + [pl.BlockSpec(memory_space=pl.ANY)] * len(partial),
        out_specs=pl.BlockSpec((rows // steps, N2, held), lambda s: (s, 0, lax.axis_index("bat") ^ other)),
        scratch_shapes=[pltpu.VMEM((2, rows * (held + PAD), 128), jnp.float32)],
        out_shape=jax.ShapeDtypeStruct((rows, N2, channels), jnp.bfloat16),
        input_output_aliases={len(received): 0} if partial else {},
        compiler_params=pltpu.CompilerParams(vmem_limit_bytes=12 * 1024 * 1024),
    )(*inputs)


def cross(far, count):
    half = count // 2
    received = []
    for step, block in enumerate(far):
        received.append(lax.ppermute(block, "seq", [(s, s ^ (half + step)) for s in range(count)]))
    return received


def near(kept, count):
    half = count // 2
    halves = [list(range(half)), list(range(half, count))]
    return lax.all_to_all(kept, "seq", split_axis=0, concat_axis=0, tiled=True, axis_index_groups=halves)


def swap(array):
    return lax.ppermute(array, "bat", [(0, 1), (1, 0)])


def direct_body(tokens, filter_spectrum, skip_gain):
    count = lax.axis_size("seq")
    groups = lax.axis_size("bat")
    index = lax.axis_index("seq")
    _, local_length, channels = tokens.shape
    rows = N1 // count
    half = count // 2
    laid = tokens.reshape(rows, N2, channels)
    kept, *far = pack_tokens(laid, half, groups, 0)
    far_own = cross(far, count)
    kept, *far = pack_filters(filter_spectrum, kept, half)
    far_filters = cross(far, count)
    kept_own = near(kept, count)
    kept, *far = pack_tokens(laid, half, groups, 1)
    far_other = cross(far, count)
    kept_other = near(kept, count)
    *tables, final_t = dft_tables(relative_rows(index, count, rows))
    tables.append(jnp.concatenate([final_t[0], final_t[1]], axis=1))
    (ready,) = transform(skip_gain, kept_own, far_own, tables, far_filters, 0, True)
    first = lax.all_to_all(ready, "seq", split_axis=0, concat_axis=0, tiled=True)
    gathered = gather(far_filters)
    filters = (swap(kept_own), swap(gathered))
    kept, *far = transform(skip_gain, kept_other, far_other, tables, filters, 1, False)
    far = cross(far, count)
    kept = near(kept, count)
    mixed = unpack([first], rows, channels, groups, half, 0, [])
    mixed = unpack([kept, *far], rows, channels, groups, half, 1, [mixed])
    return mixed.reshape(1, local_length, channels)


def direct_fits(tokens, count, groups):
    batch_rows, _, channels = tokens.shape
    power = count > 2 and count & (count - 1) == 0
    return power and groups == 2 and batch_rows == 1 and N1 // count % 16 == 0 and channels // groups % (LANES * count) == 0


def body(tokens, filter_spectrum, skip_gain):
    if direct_fits(tokens, lax.axis_size("seq"), lax.axis_size("bat")):
        return direct_body(tokens, filter_spectrum, skip_gain)
    return spread_body(tokens, filter_spectrum, skip_gain)


def solution(mesh):
    placed = (P("bat", "seq", None), P(None, "seq", None, "bat"), P())
    return jax.shard_map(
        body, mesh=mesh, in_specs=placed, out_specs=P("bat", "seq", None), check_vma=False
    )
```
